512 devices in a mesh: obs: 2 (over y), bt: 16 (over z), freq: 8 (over x), pol: 2 (over core).
Axes of the slice: x: 8, y: 2, z: 16, core: 2. Of those that a mesh axis runs over, the one named last changes fastest.
The devices are a block of a 8x8x16 slice.
Arguments:
- gains: float32 [64, 16, 8, 7936], P(('obs', 'bt', 'pol'), 'freq'), parts along dimension 0, may hold values from -3 to 3
- visibilities: bfloat16 [64, 16, 8, 16384], P('obs', 'freq', None, ('bt', 'pol')), parts along dimension 0, may hold values from -6 to 6
- first_station: int32 [32768], P(('obs', 'bt', 'pol')), parts along dimension 0, may hold values from 0 to 61
- second_station: int32 [32768], P(('obs', 'bt', 'pol')), parts along dimension 0, may hold values from 0 to 61, as said below
- filled_row_count: int32 [64], P(('obs', 'bt', 'pol')), parts along dimension 0, may hold values from 256 to 512
- facet_dir: int32 [64], P('obs'), parts along dimension 0, may hold values from 0 to 31, each once
Outputs:
- corrected: bfloat16 [64, 16, 8, 16384], P('obs', 'freq', None, ('bt', 'pol')), parts along dimension 0
The draws below stay inside these ranges and needn't reach their ends.
There are 2 independent parts, one for each index of `obs`. The reference program is written for one: setup_inputs(seed, part) draws one part's arguments, and reference() takes and returns one part's arrays. A program takes and returns all parts, laid end to end along the dimension named above; each array names one. Nothing has to cross between parts.
Inputs may be any that keep to these rules, and one draw needn't show every extreme that they name: In every row second_station differs from first_station. `facet_dir`: each direction names exactly one facet.
All inputs are finite; a program needn't handle non-finite values.
Results may differ from the reference program's by a relative error of at most 0.001.
Values sent between devices are 32-bit elements; how exact they have to be, the bound alone decides.
A program may use at most 64 MiB of HBM per device.

```python
import jax
import jax.numpy as jnp
from jax import lax

ARRAY_STATIONS = 62
GAIN_SLOT_COUNT = 4
BLOCK_ROW_COUNT = 512
BLOCKS = 32
DIRS = 32
FACETS = 32
CHANS = 16
TIMES = 128
ROWS = 16384


def station_pair(key):
    folded = jax.random.fold_in(key, 17)
    first_key, second_key = jax.random.split(folded)
    first = jax.random.randint(first_key, (ROWS,), 0, ARRAY_STATIONS, dtype=jnp.int32)
    offset = jax.random.randint(second_key, (ROWS,), 1, ARRAY_STATIONS, dtype=jnp.int32)
    return (first, (first + offset) % ARRAY_STATIONS)


def draw_first_station(key, part):
    return station_pair(key)[0]


def draw_second_station(key, part):
    return station_pair(key)[1]


def with_ends(array, stream_key, low, largest):
    longest = array.shape.index(max(array.shape))
    spots = []
    for shift in (0, 1):
        where = [jax.random.randint(jax.random.fold_in(stream_key, axis), (), 0, length) for axis, length in enumerate(array.shape)]
        where[longest] = (where[longest] + shift) % array.shape[longest]
        spots.append(tuple(where))
    return array.at[spots[0]].set(low).at[spots[1]].set(largest)


def levels(rng, shape, pieces, low, largest):
    def one(dim, shards_of):
        heights = jax.random.uniform(jax.random.fold_in(jax.random.fold_in(rng, 6), dim), (shards_of,), jnp.float32, low / len(pieces), largest / len(pieces))
        return jnp.repeat(jnp.exp(heights), shape[dim] // shards_of).reshape((-1,) + (1,) * (len(shape) - dim - 1))

    level = one(*pieces[0])
    for cut in pieces[1:]:
        level = level * one(*cut)
    return level


def centred(own_key, shape, spread, most, cuts=(), kind=jnp.bfloat16):
    level = levels(own_key, shape, cuts, -0.22, 0.18) if cuts else 1.0
    result = jax.random.normal(own_key, shape, jnp.float32) * spread * level
    return jnp.minimum(jnp.maximum(result, -most), most).astype(kind)


def setup_inputs(seed: int = 0, part: int = 0) -> dict:
    streams_of = jax.random.split(jax.random.key(seed), 7)
    part_keys = jax.random.split(jax.random.fold_in(streams_of[6], part), 7)
    gains = centred(part_keys[0], (DIRS, CHANS, 8, TIMES * ARRAY_STATIONS), 0.5, 3.0, ((0, 32), (1, 8)), jnp.float32)
    visibilities = centred(part_keys[1], (FACETS, CHANS, 8, ROWS), 1.0, 6.0, ((1, 8), (3, 32)))
    first_station = draw_first_station(jax.random.fold_in(jax.random.fold_in(streams_of[6], part), 71), part)
    second_station = draw_second_station(jax.random.fold_in(jax.random.fold_in(streams_of[6], part), 71), part)
    filled_row_count = with_ends(jax.random.randint(part_keys[4], (BLOCKS,), BLOCK_ROW_COUNT // 2, BLOCK_ROW_COUNT + 1), jax.random.fold_in(part_keys[4], 1), BLOCK_ROW_COUNT // 2, BLOCK_ROW_COUNT).astype(jnp.int32)
    facet_dir = jax.random.permutation(part_keys[5], DIRS).astype(jnp.int32)
    return dict(gains=gains, visibilities=visibilities, first_station=first_station, second_station=second_station, filled_row_count=filled_row_count, facet_dir=facet_dir)


def entry(values, row_at, col_at):
    return values[..., 2 * row_at + col_at, :], values[..., 4 + 2 * row_at + col_at, :]


def apply_jones(left_matrix, data, right_matrix):
    real_parts = []
    imag_parts = []
    for out_row in (0, 1):
        for out_col in (0, 1):
            total_re = jnp.zeros_like(left_matrix[..., 0, :])
            total_im = jnp.zeros_like(left_matrix[..., 0, :])
            for middle in (0, 1):
                for column in (0, 1):
                    left_re, left_im = entry(left_matrix, out_row, middle)
                    data_re, data_im = entry(data, middle, column)
                    right_re, right_im = entry(right_matrix, out_col, column)
                    prod_re = left_re * data_re - left_im * data_im
                    prod_im = left_re * data_im + left_im * data_re
                    total_re = total_re + prod_re * right_re + prod_im * right_im
                    total_im = total_im + prod_im * right_re - prod_re * right_im
            real_parts.append(total_re)
            imag_parts.append(total_im)
    return jnp.stack(real_parts + imag_parts, axis=-2)


def slot_blend_weight(antenna, block_rows, slots, stations):
    row_ids = jnp.arange(block_rows, dtype=jnp.int32)
    per_slot = block_rows // slots
    row_slot = row_ids // per_slot
    fraction = ((row_ids % per_slot).astype(jnp.float32) + 0.5) / per_slot
    slot_ids = jnp.arange(slots + 1, dtype=jnp.int32)[:, None, None]
    station_ids = jnp.arange(stations, dtype=jnp.int32)[None, :, None]
    time_weight = jnp.where(slot_ids == row_slot[None, None, :], 1.0 - fraction, 0.0 * fraction)
    time_weight = time_weight + jnp.where(slot_ids == row_slot[None, None, :] + 1, fraction, 0.0 * fraction)
    station_mask = (station_ids == antenna[None, None, :]).astype(jnp.float32)
    weights_table = time_weight * station_mask
    return weights_table.reshape((slots + 1) * stations, block_rows)


def apply_correction(gain_window, block_visibilities, first_station_gain, second_station_gain, filled_rows):
    block_rows = block_visibilities.shape[3]
    left_matrix = jnp.einsum("hsxv,va->hsxa", gain_window, slot_blend_weight(first_station_gain, block_rows, GAIN_SLOT_COUNT, ARRAY_STATIONS), precision=lax.Precision.HIGHEST)
    right_matrix = jnp.einsum("hsxv,va->hsxa", gain_window, slot_blend_weight(second_station_gain, block_rows, GAIN_SLOT_COUNT, ARRAY_STATIONS), precision=lax.Precision.HIGHEST)
    product = apply_jones(left_matrix, block_visibilities.astype(jnp.float32), right_matrix)
    live_mask = jnp.arange(block_rows, dtype=jnp.int32) < filled_rows
    return jnp.where(live_mask, product, 0.0 * product).astype(jnp.bfloat16)


def reference(gains, visibilities, first_station, second_station, filled_row_count, facet_dir):
    onehot = (facet_dir[:, None] == jnp.arange(DIRS, dtype=jnp.int32)[None, :]).astype(jnp.float32)
    chosen = jnp.einsum("fd,dckn->fckn", onehot, gains, precision=lax.Precision.HIGHEST)
    final_slot = chosen[..., (TIMES - 1) * ARRAY_STATIONS:]
    extended = jnp.concatenate([chosen, final_slot], axis=3)

    def one_block(block_index):
        gain_window = lax.dynamic_slice_in_dim(extended, block_index * (GAIN_SLOT_COUNT * ARRAY_STATIONS), (GAIN_SLOT_COUNT + 1) * ARRAY_STATIONS, 3)
        block_visibilities = lax.dynamic_slice_in_dim(visibilities, block_index * BLOCK_ROW_COUNT, BLOCK_ROW_COUNT, 3)
        first_station_gain = lax.dynamic_slice_in_dim(first_station, block_index * BLOCK_ROW_COUNT, BLOCK_ROW_COUNT, 0)
        second_station_gain = lax.dynamic_slice_in_dim(second_station, block_index * BLOCK_ROW_COUNT, BLOCK_ROW_COUNT, 0)
        return apply_correction(gain_window, block_visibilities, first_station_gain, second_station_gain, filled_row_count[block_index])

    blocks_out = lax.map(one_block, jnp.arange(BLOCKS, dtype=jnp.int32))
    blocks_out = jnp.moveaxis(blocks_out, 0, 3)
    return blocks_out.reshape(FACETS, CHANS, 8, ROWS)
```

```python
import functools

import jax
import jax.numpy as jnp
from jax import lax
from jax.experimental import pallas as pl
from jax.experimental.pallas import tpu as pltpu
from jax.sharding import PartitionSpec as P

ARRAY_STATIONS = 62
GAIN_SLOT_COUNT = 4
LANES = 128
TILES = 5
MESH = pl.DeviceIdType.MESH


def gather_lanes(tile, index):
    return jnp.take_along_axis(tile, index, axis=1, mode="promise_in_bounds")


def window(held, chan, start):
    tile, shift = divmod(start, LANES)
    here = held[chan, :, tile * LANES : (tile + 1) * LANES]
    if shift == 0:
        return here
    lane = lax.broadcasted_iota(jnp.int32, here.shape, 1)
    if (tile + 1) * LANES < held.shape[2]:
        after = held[chan, :, (tile + 1) * LANES : (tile + 2) * LANES]
        here = jnp.where(lane >= shift, here, after)
    return pltpu.roll(here, LANES - shift, 1)


def kernel(
    peers,
    bt_count,
    pol_count,
    filled_ref,
    facet_dir_ref,
    first_ref,
    second_ref,
    gains_hbm,
    vis_hbm,
    out_ref,
    held,
    outgoing,
    incoming,
    vis,
    done,
    left_rows,
    right_rows,
    data_rows,
    out_rows,
    gains_sem,
    vis_sem,
    send_sem,
    recv_sem,
):
    chans = held.shape[0]
    slots = GAIN_SLOT_COUNT
    rotate = jnp.where((lax.axis_index("obs") == 0) & (lax.axis_index("freq") == 0), 1, 0)
    me = lax.axis_index("bt") * pol_count + lax.axis_index("pol")
    rank = lax.rem(me - rotate + peers, peers)

    def place(order):
        return lax.rem(order + rotate, peers)

    def device(where):
        return {"bt": where // pol_count, "pol": lax.rem(where, pol_count)}

    def to(where):
        return pltpu.make_async_remote_copy(
            src_ref=outgoing.at[where],
            dst_ref=incoming.at[me],
            send_sem=send_sem.at[where],
            recv_sem=recv_sem.at[me],
            device_id=device(where),
            device_id_type=MESH,
        )

    def arrival(where):
        return pltpu.make_async_remote_copy(
            src_ref=outgoing.at[where],
            dst_ref=incoming.at[where],
            send_sem=send_sem.at[where],
            recv_sem=recv_sem.at[where],
            device_id=device(where),
            device_id_type=MESH,
        )

    load_gains = pltpu.make_async_copy(gains_hbm.at[0], held, gains_sem)
    load_gains.start()
    load_vis = pltpu.make_async_copy(vis_hbm, vis, vis_sem)
    load_vis.start()

    barrier = pltpu.get_barrier_semaphore()

    @pl.when(rank > 0)
    def _():
        pl.semaphore_wait(barrier, 1)

    @pl.when(rank < peers - 1)
    def _():
        pl.semaphore_signal(barrier, inc=1, device_id=device(place(rank + 1)), device_id_type=MESH)

    load_gains.wait()
    lane = lax.broadcasted_iota(jnp.int32, (8, LANES), 1)
    total_slots = peers * slots
    for where in range(peers):
        base = where * slots
        for chan in range(chans):
            for half in range(2):
                outgoing[where, chan * 2 + half] = window(held, chan, (base + 2 * half) * ARRAY_STATIONS)
        last = min(base + slots, total_slots - 1) * ARRAY_STATIONS
        outgoing[where, 2 * chans] = jnp.where(
            lane < LANES // 2, window(held, 0, last), pltpu.roll(window(held, 1, last), LANES // 2, 1)
        )
    incoming[me] = outgoing[me]

    def send_down(order, carry):
        to(place(order)).start()
        return carry

    lax.fori_loop(0, rank, send_down, 0)

    unit = lax.broadcasted_iota(jnp.int32, (8, LANES), 0)
    slot_of_unit = lax.rem(unit, slots)
    live = slot_of_unit * LANES + lane < filled_ref[0]
    after = (lane.astype(jnp.float32) + 0.5) / LANES
    before = 1.0 - after
    load_vis.wait()

    def spread(where, ref, rows):
        for slot in range(slots):
            station = jnp.broadcast_to(ref[slot : slot + 1, :], (8, LANES))
            upper = station + ARRAY_STATIONS
            for chan in range(chans):
                now = incoming[where, chan * 2 + slot // 2]
                if slot % 2 == 0:
                    low, high = gather_lanes(now, station), gather_lanes(now, upper)
                else:
                    low = gather_lanes(now, upper)
                    if slot + 1 < slots:
                        high = gather_lanes(incoming[where, chan * 2 + slot // 2 + 1], station)
                    else:
                        high = gather_lanes(incoming[where, 2 * chans], station + chan * (LANES // 2))
                at = (chan * slots + slot) * 8
                rows[at : at + 8, :] = before * low + after * high

    def component(rows, k):
        return rows[pl.ds(k, 8, stride=8), :]

    def correct(where):
        spread(where, first_ref, left_rows)
        spread(where, second_ref, right_rows)
        left = [component(left_rows, k) for k in range(8)]
        right = [component(right_rows, k) for k in range(8)]
        data = [component(data_rows, k) for k in range(8)]
        for row in (0, 1):
            half_re, half_im = [], []
            for column in (0, 1):
                re = im = None
                for middle in (0, 1):
                    l_re, l_im = left[2 * row + middle], left[4 + 2 * row + middle]
                    d_re, d_im = data[2 * middle + column], data[4 + 2 * middle + column]
                    p_re = l_re * d_re - l_im * d_im
                    p_im = l_re * d_im + l_im * d_re
                    re = p_re if re is None else re + p_re
                    im = p_im if im is None else im + p_im
                half_re.append(re)
                half_im.append(im)
            for out in (0, 1):
                re = im = None
                for column in (0, 1):
                    r_re, r_im = right[2 * out + column], right[4 + 2 * out + column]
                    p_re = half_re[column] * r_re + half_im[column] * r_im
                    p_im = half_im[column] * r_re - half_re[column] * r_im
                    re = p_re if re is None else re + p_re
                    im = p_im if im is None else im + p_im
                out_rows[pl.ds(2 * row + out, 8, stride=8), :] = jnp.where(live, re, 0.0)
                out_rows[pl.ds(4 + 2 * row + out, 8, stride=8), :] = jnp.where(live, im, 0.0)
        for chan in range(chans):
            for slot in range(slots):
                at = (chan * slots + slot) * 8
                done[where, chan, :, slot * LANES : (slot + 1) * LANES] = out_rows[at : at + 8, :].astype(done.dtype)

    def step(order, carry):
        where = place(order)
        facet = jnp.int32(0)
        for f in range(peers):
            facet = jnp.where(facet_dir_ref[f] == where, f, facet)
        for chan in range(chans):
            for slot in range(slots):
                at = (chan * slots + slot) * 8
                data_rows[at : at + 8, :] = vis[facet, chan, :, slot * LANES : (slot + 1) * LANES].astype(jnp.float32)

        @pl.when(order != rank)
        def _():
            arrival(where).wait_recv()

        @pl.when(order > rank)
        def _():
            to(where).start()

        correct(where)
        return carry

    lax.fori_loop(0, peers, step, 0)

    def finish(order, carry):
        @pl.when(order != rank)
        def _():
            to(place(order)).wait_send()

        return carry

    lax.fori_loop(0, peers, finish, 0)
    for f in range(peers):
        out_ref[f] = done[facet_dir_ref[f]]


def shards(gains, visibilities, first_station, second_station, filled_row_count, facet_dir):
    bt_count, pol_count = lax.axis_size("bt"), lax.axis_size("pol")
    peers = bt_count * pol_count
    chans = gains.shape[1]
    any_spec = pl.BlockSpec(memory_space=pl.ANY)
    smem = pl.BlockSpec(memory_space=pltpu.SMEM)
    vmem = pl.BlockSpec(memory_space=pltpu.VMEM)
    rows = 8 * chans * GAIN_SLOT_COUNT
    return pl.pallas_call(
        functools.partial(kernel, peers, bt_count, pol_count),
        name="correct",
        out_shape=jax.ShapeDtypeStruct(visibilities.shape, visibilities.dtype),
        in_specs=[smem, smem, vmem, vmem, any_spec, any_spec],
        out_specs=vmem,
        scratch_shapes=[
            pltpu.VMEM(gains.shape[1:], jnp.float32),
            pltpu.VMEM((peers, TILES, 8, LANES), jnp.float32),
            pltpu.VMEM((peers, TILES, 8, LANES), jnp.float32),
            pltpu.VMEM(visibilities.shape, visibilities.dtype),
            pltpu.VMEM(visibilities.shape, visibilities.dtype),
            pltpu.VMEM((rows, LANES), jnp.float32),
            pltpu.VMEM((rows, LANES), jnp.float32),
            pltpu.VMEM((rows, LANES), jnp.float32),
            pltpu.VMEM((rows, LANES), jnp.float32),
            pltpu.SemaphoreType.DMA,
            pltpu.SemaphoreType.DMA,
            pltpu.SemaphoreType.DMA((peers,)),
            pltpu.SemaphoreType.DMA((peers,)),
        ],
        compiler_params=pltpu.CompilerParams(collective_id=0, has_side_effects=True),
    )(
        filled_row_count,
        facet_dir,
        first_station.reshape(GAIN_SLOT_COUNT, LANES),
        second_station.reshape(GAIN_SLOT_COUNT, LANES),
        gains,
        visibilities,
    )


def solution(mesh):
    return jax.shard_map(
        shards,
        mesh=mesh,
        in_specs=(
            P(("obs", "bt", "pol"), "freq", None, None),
            P("obs", "freq", None, ("bt", "pol")),
            P(("obs", "bt", "pol")),
            P(("obs", "bt", "pol")),
            P(("obs", "bt", "pol")),
            P("obs"),
        ),
        out_specs=P("obs", "freq", None, ("bt", "pol")),
        check_vma=False,
    )
```

```python
import functools

import jax
import jax.numpy as jnp
from jax import lax
from jax.experimental import pallas as pl
from jax.experimental.pallas import tpu as pltpu
from jax.sharding import PartitionSpec as P

ARRAY_STATIONS = 62
GAIN_SLOT_COUNT = 4
LANES = 128
TILES = 5
IN_FLIGHT = 2
URGENT_LAYERS = 2
LATE_LAYERS = 3
LAG = 4
MESH = pl.DeviceIdType.MESH


def gather_lanes(tile, index):
    return jnp.take_along_axis(tile, index, axis=1, mode="promise_in_bounds")


def window(held, chan, start):
    tile, shift = divmod(start, LANES)
    here = held[chan, :, tile * LANES : (tile + 1) * LANES]
    if shift == 0:
        return here
    lane = lax.broadcasted_iota(jnp.int32, here.shape, 1)
    if (tile + 1) * LANES < held.shape[2]:
        after = held[chan, :, (tile + 1) * LANES : (tile + 2) * LANES]
        here = jnp.where(lane >= shift, here, after)
    return pltpu.roll(here, LANES - shift, 1)


def kernel(
    peers,
    bt_count,
    pol_count,
    filled_ref,
    facet_dir_hbm,
    first_hbm,
    second_hbm,
    gains_hbm,
    vis_hbm,
    out_ref,
    facet_dir_ref,
    first_ref,
    second_ref,
    held,
    outgoing,
    incoming,
    vis,
    done,
    left_rows,
    right_rows,
    data_rows,
    out_rows,
    load_sem,
    urgent_sem,
    send_sem,
    recv_sem,
    entered,
    go,
):
    chans = held.shape[0]
    slots = GAIN_SLOT_COUNT
    layers, half = peers // pol_count, bt_count // 2
    rotate = jnp.where((lax.axis_index("obs") == 0) & (lax.axis_index("freq") == 0), 1, 0)
    rank = lax.rem(lax.axis_index("bt") * pol_count + lax.axis_index("pol") + peers - rotate, peers)
    layer = rank // pol_count
    partner = layer * pol_count + lax.rem(rank + 1, pol_count)

    def place(order):
        return lax.rem(order + rotate, peers)

    def device(order):
        where = place(order)
        return {"bt": where // pol_count, "pol": lax.rem(where, pol_count)}

    def to(order, sem):
        return pltpu.make_async_remote_copy(
            src_ref=outgoing.at[place(order)],
            dst_ref=incoming.at[rank],
            send_sem=sem,
            recv_sem=recv_sem.at[layer],
            device_id=device(order),
            device_id_type=MESH,
        )

    def transfers(start, count, sem, into):
        return pltpu.make_async_remote_copy(
            src_ref=outgoing.at[pl.ds(start, count)],
            dst_ref=incoming.at[pl.ds(start, count)],
            send_sem=sem,
            recv_sem=recv_sem.at[into],
            device_id=device(partner),
            device_id_type=MESH,
        )

    def signal(sem, order):
        pl.semaphore_signal(sem, inc=1, device_id=device(order), device_id_type=MESH)

    loads = [
        pltpu.make_async_copy(source, target, load_sem.at[i])
        for i, (source, target) in enumerate(
            (
                (gains_hbm.at[0], held),
                (first_hbm, first_ref),
                (second_hbm, second_ref),
                (facet_dir_hbm, facet_dir_ref),
                (vis_hbm, vis),
            )
        )
    ]
    for load in loads:
        load.start()

    barrier = pltpu.get_barrier_semaphore()

    @pl.when(rank > 0)
    def _():
        with jax.named_scope("chain"):
            pl.semaphore_wait(barrier, 1)

    @pl.when(rank < peers - 1)
    def _():
        signal(barrier, rank + 1)

    def greet(order, carry):
        signal(entered.at[layer], order)
        return carry

    lax.fori_loop(0, rank, greet, 0)

    with jax.named_scope("gains"):
        loads[0].wait()
    lane = lax.broadcasted_iota(jnp.int32, (8, LANES), 1)
    total_slots = peers * slots
    urgent = URGENT_LAYERS * pol_count

    def pack(where):
        base = where * slots
        for chan in range(chans):
            for half in range(2):
                outgoing[where, chan * 2 + half] = window(held, chan, (base + 2 * half) * ARRAY_STATIONS)
        last = min(base + slots, total_slots - 1) * ARRAY_STATIONS
        outgoing[where, 2 * chans] = jnp.where(
            lane < LANES // 2, window(held, 0, last), pltpu.roll(window(held, 1, last), LANES // 2, 1)
        )

    def send(order, carry):
        to(order, send_sem).start()
        return carry

    def hasten(order, carry):
        to(order, urgent_sem.at[order]).start()
        return carry

    def hasten_next(order, carry):
        to(order - IN_FLIGHT, urgent_sem.at[order - IN_FLIGHT]).wait_send()
        return hasten(order, carry)

    def hastened(order, carry):
        to(order, urgent_sem.at[order]).wait_send()
        return carry

    hurry = jnp.minimum(rank, urgent)
    for where in range(urgent + 1):
        pack(where)
    with jax.named_scope("urgent"):
        lax.fori_loop(0, jnp.minimum(rank, IN_FLIGHT), hasten, 0)
        for where in range(urgent + 1, peers):
            pack(where)
        lax.fori_loop(IN_FLIGHT, hurry, hasten_next, 0)
        lax.fori_loop(jnp.maximum(hurry - IN_FLIGHT, 0), hurry, hastened, 0)

    late = layers - LATE_LAYERS
    far_above = jnp.where(rank < urgent, layers, jnp.minimum(jnp.maximum(layer + half, late), layers))
    far_below = jnp.where(layer < late, URGENT_LAYERS, jnp.maximum(layer - half + 1, URGENT_LAYERS))

    def send_far():
        @pl.when((rank >= urgent) & (layer < half))
        def _():
            with jax.named_scope("go"):
                pl.semaphore_wait(go, 1)
            lax.fori_loop(far_above * pol_count, peers, send, 0)

        @pl.when((layer >= late) & (layer < layers - 1))
        def _():
            def turn_of(low, carry):
                with jax.named_scope("go"):
                    pl.semaphore_wait(go, 1)
                for core in range(pol_count):
                    send(low * pol_count + core, 0)
                return carry

            lax.fori_loop(URGENT_LAYERS, far_below, turn_of, 0)

        @pl.when(layer == layers - 1)
        def _():
            def turn_of(low, carry):
                @pl.when(rank == peers - pol_count)
                def _():
                    for core in range(pol_count):
                        signal(go, low * pol_count + core)

                    def release(order, carry):
                        signal(go, order)
                        return carry

                    lax.fori_loop(jnp.maximum(low + half, late) * pol_count, peers - pol_count, release, 0)

                for core in range(pol_count):
                    to(low * pol_count + core, urgent_sem.at[core]).start()
                for core in range(pol_count):
                    to(low * pol_count + core, urgent_sem.at[core]).wait_send()
                return carry

            lax.fori_loop(URGENT_LAYERS, far_below, turn_of, 0)

    incoming[rank] = outgoing[place(rank)]
    with jax.named_scope("loads"):
        for load in loads[1:]:
            load.wait()

    unit = lax.broadcasted_iota(jnp.int32, (8, LANES), 0)
    slot_of_unit = lax.rem(unit, slots)
    live = slot_of_unit * LANES + lane < filled_ref[0]
    after = (lane.astype(jnp.float32) + 0.5) / LANES
    before = 1.0 - after

    def spread(where, ref, rows):
        for slot in range(slots):
            station = jnp.broadcast_to(ref[slot : slot + 1, :], (8, LANES))
            upper = station + ARRAY_STATIONS
            for chan in range(chans):
                now = incoming[where, chan * 2 + slot // 2]
                if slot % 2 == 0:
                    low, high = gather_lanes(now, station), gather_lanes(now, upper)
                else:
                    low = gather_lanes(now, upper)
                    if slot + 1 < slots:
                        high = gather_lanes(incoming[where, chan * 2 + slot // 2 + 1], station)
                    else:
                        high = gather_lanes(incoming[where, 2 * chans], station + chan * (LANES // 2))
                at = (chan * slots + slot) * 8
                rows[at : at + 8, :] = before * low + after * high

    def component(rows, k):
        return rows[pl.ds(k, 8, stride=8), :]

    def correct(order, where):
        spread(order, first_ref, left_rows)
        spread(order, second_ref, right_rows)
        left = [component(left_rows, k) for k in range(8)]
        right = [component(right_rows, k) for k in range(8)]
        data = [component(data_rows, k) for k in range(8)]
        for row in (0, 1):
            half_re, half_im = [], []
            for column in (0, 1):
                re = im = None
                for middle in (0, 1):
                    l_re, l_im = left[2 * row + middle], left[4 + 2 * row + middle]
                    d_re, d_im = data[2 * middle + column], data[4 + 2 * middle + column]
                    p_re = l_re * d_re - l_im * d_im
                    p_im = l_re * d_im + l_im * d_re
                    re = p_re if re is None else re + p_re
                    im = p_im if im is None else im + p_im
                half_re.append(re)
                half_im.append(im)
            for out in (0, 1):
                re = im = None
                for column in (0, 1):
                    r_re, r_im = right[2 * out + column], right[4 + 2 * out + column]
                    p_re = half_re[column] * r_re + half_im[column] * r_im
                    p_im = half_im[column] * r_re - half_re[column] * r_im
                    re = p_re if re is None else re + p_re
                    im = p_im if im is None else im + p_im
                out_rows[pl.ds(2 * row + out, 8, stride=8), :] = jnp.where(live, re, 0.0)
                out_rows[pl.ds(4 + 2 * row + out, 8, stride=8), :] = jnp.where(live, im, 0.0)
        for chan in range(chans):
            for slot in range(slots):
                at = (chan * slots + slot) * 8
                done[where, chan, :, slot * LANES : (slot + 1) * LANES] = out_rows[at : at + 8, :].astype(done.dtype)

    def take(order):
        where = place(order)
        facet = jnp.int32(0)
        for f in range(peers):
            facet = jnp.where(facet_dir_ref[f] == where, f, facet)
        for chan in range(chans):
            for slot in range(slots):
                at = (chan * slots + slot) * 8
                data_rows[at : at + 8, :] = vis[facet, chan, :, slot * LANES : (slot + 1) * LANES].astype(jnp.float32)
        correct(order, where)

    with jax.named_scope("own"):
        take(rank)
    above = layers - 1 - layer
    near_above = far_above - 1 - layer

    def answer(turn, carry):
        @pl.when((turn == 0) & (rank < partner))
        def _():
            pl.semaphore_wait(entered.at[layer], pol_count - 1)
            send(partner, 0)

        @pl.when((turn == 0) & (rank > partner) & (rank >= urgent))
        def _():
            send(partner, 0)

        @pl.when((turn > 0) & (turn <= above))
        def _():
            with jax.named_scope("hello"):
                pl.semaphore_wait(entered.at[layer + turn], pol_count)

            @pl.when(layer + turn < far_above)
            def _():
                for core in range(pol_count):
                    send((layer + turn) * pol_count + core, 0)

        first = jnp.where(turn == 0, far_below, far_below + turn + 1)
        last = jnp.where(turn < above, jnp.minimum(far_below + turn + 2, layer), jnp.where(turn == above, layer, 0))

        def send_near(low, carry):
            for core in range(pol_count):
                send(low * pol_count + core, 0)
            return carry

        lax.fori_loop(first, last, send_near, 0)

        @pl.when(turn == above)
        def _():
            send_far()

        step = turn - LAG

        @pl.when(step == 0)
        def _():
            transfers(partner, pol_count - 1, send_sem, layer).wait_recv()
            take(partner)

        @pl.when(step > 0)
        def _():
            source = jnp.where(step <= near_above, layer + step, step)
            source = jnp.where((step > near_above) & (step <= near_above + layer), step - near_above - 1, source)
            with jax.named_scope("arrive"):
                transfers(source * pol_count, pol_count, send_sem, source).wait_recv()
            with jax.named_scope("correct"):

                def both(core, carry):
                    take(source * pol_count + core)
                    return carry

                lax.fori_loop(0, pol_count, both, 0)

        return carry

    lax.fori_loop(0, layers + LAG, answer, 0)

    with jax.named_scope("finish"):
        paced = (half - URGENT_LAYERS) * pol_count
        for count in range(urgent + 1):

            @pl.when((hurry == count) & (layer < layers - 1))
            def _():
                transfers(0, peers - 1 - count, send_sem, layer).wait_send()

        @pl.when(layer == layers - 1)
        def _():
            transfers(0, peers - 1 - urgent - paced, send_sem, layer).wait_send()

    with jax.named_scope("order"):
        for f in range(peers):
            out_ref[f] = done[facet_dir_ref[f]]


def shards(gains, visibilities, first_station, second_station, filled_row_count, facet_dir):
    bt_count, pol_count = lax.axis_size("bt"), lax.axis_size("pol")
    peers = bt_count * pol_count
    chans = gains.shape[1]
    hbm = pl.BlockSpec(memory_space=pltpu.HBM)
    vmem = pl.BlockSpec(memory_space=pltpu.VMEM)
    rows = 8 * chans * GAIN_SLOT_COUNT
    operands = (
        facet_dir,
        first_station.reshape(GAIN_SLOT_COUNT, LANES),
        second_station.reshape(GAIN_SLOT_COUNT, LANES),
        gains,
        visibilities,
    )
    return pl.pallas_call(
        functools.partial(kernel, peers, bt_count, pol_count),
        name="correct",
        out_shape=jax.ShapeDtypeStruct(visibilities.shape, visibilities.dtype),
        in_specs=[pl.BlockSpec(memory_space=pltpu.SMEM)] + [hbm] * 5,
        out_specs=vmem,
        scratch_shapes=[
            pltpu.SMEM(facet_dir.shape, jnp.int32),
            pltpu.VMEM((GAIN_SLOT_COUNT, LANES), jnp.int32),
            pltpu.VMEM((GAIN_SLOT_COUNT, LANES), jnp.int32),
            pltpu.VMEM(gains.shape[1:], jnp.float32),
            pltpu.VMEM((peers, TILES, 8, LANES), jnp.float32),
            pltpu.VMEM((peers, TILES, 8, LANES), jnp.float32),
            pltpu.VMEM(visibilities.shape, visibilities.dtype),
            pltpu.VMEM(visibilities.shape, visibilities.dtype),
            pltpu.VMEM((rows, LANES), jnp.float32),
            pltpu.VMEM((rows, LANES), jnp.float32),
            pltpu.VMEM((rows, LANES), jnp.float32),
            pltpu.VMEM((rows, LANES), jnp.float32),
            pltpu.SemaphoreType.DMA((5,)),
            pltpu.SemaphoreType.DMA((URGENT_LAYERS * pol_count,)),
            pltpu.SemaphoreType.DMA,
            pltpu.SemaphoreType.DMA((bt_count,)),
            pltpu.SemaphoreType.REGULAR((bt_count,)),
            pltpu.SemaphoreType.REGULAR,
        ],
        compiler_params=pltpu.CompilerParams(collective_id=0, has_side_effects=True, vmem_limit_bytes=8 << 20),
    )(filled_row_count, *(pltpu.with_memory_space_constraint(x, pltpu.HBM) for x in operands))


def solution(mesh):
    return jax.shard_map(
        shards,
        mesh=mesh,
        in_specs=(
            P(("obs", "bt", "pol"), "freq", None, None),
            P("obs", "freq", None, ("bt", "pol")),
            P(("obs", "bt", "pol")),
            P(("obs", "bt", "pol")),
            P(("obs", "bt", "pol")),
            P("obs"),
        ),
        out_specs=P("obs", "freq", None, ("bt", "pol")),
        check_vma=False,
    )
```

```python
import functools

import jax
import jax.numpy as jnp
from jax import lax
from jax.experimental import pallas as pl
from jax.experimental.pallas import tpu as pltpu
from jax.sharding import PartitionSpec as P

ARRAY_STATIONS = 62
GAIN_SLOT_COUNT = 4
LANES = 128
TILES = 5
IN_FLIGHT = 2
FREE_LAYERS = 3
LAG = 4
LAST_GO = 4
LOOK_AHEAD = 1
EARLY = 4
MESH = pl.DeviceIdType.MESH


def gather_lanes(tile, index):
    return jnp.take_along_axis(tile, index, axis=1, mode="promise_in_bounds")


def window(held, chan, start):
    tile, shift = divmod(start, LANES)
    here = held[chan, :, tile * LANES : (tile + 1) * LANES]
    if shift == 0:
        return here
    lane = lax.broadcasted_iota(jnp.int32, here.shape, 1)
    if (tile + 1) * LANES < held.shape[2]:
        after = held[chan, :, (tile + 1) * LANES : (tile + 2) * LANES]
        here = jnp.where(lane >= shift, here, after)
    return pltpu.roll(here, LANES - shift, 1)


def kernel(
    peers,
    bt_count,
    pol_count,
    filled_ref,
    facet_dir_hbm,
    first_hbm,
    second_hbm,
    gains_hbm,
    vis_hbm,
    out_ref,
    facet_dir_ref,
    first_ref,
    second_ref,
    held,
    outgoing,
    incoming,
    vis,
    done,
    left_rows,
    right_rows,
    data_rows,
    out_rows,
    load_sem,
    urgent_sem,
    send_sem,
    recv_sem,
    entered,
    go,
):
    chans = held.shape[0]
    slots = GAIN_SLOT_COUNT
    layers, half = peers // pol_count, bt_count // 2
    own_place = lax.axis_index("bt") * pol_count + lax.axis_index("pol")
    behind = (layers - 2) * pol_count - 1
    shifted = (lax.axis_index("obs") == 0) & (lax.axis_index("freq") == 0)
    rank = jnp.where(own_place == 0, behind, jnp.where(own_place <= behind, own_place - 1, own_place))
    rank = jnp.where(shifted, rank, own_place)
    layer = rank // pol_count
    partner = layer * pol_count + lax.rem(rank + 1, pol_count)

    def place(order):
        moved = jnp.where(order == behind, 0, jnp.where(order < behind, order + 1, order))
        return jnp.where(shifted, moved, order)

    def device(order):
        where = place(order)
        return {"bt": where // pol_count, "pol": lax.rem(where, pol_count)}

    def to(order, sem):
        return pltpu.make_async_remote_copy(
            src_ref=outgoing.at[place(order)],
            dst_ref=incoming.at[rank],
            send_sem=sem,
            recv_sem=recv_sem.at[layer],
            device_id=device(order),
            device_id_type=MESH,
        )

    def transfers(start, count, sem, into):
        return pltpu.make_async_remote_copy(
            src_ref=outgoing.at[pl.ds(start, count)],
            dst_ref=incoming.at[pl.ds(start, count)],
            send_sem=sem,
            recv_sem=recv_sem.at[into],
            device_id=device(partner),
            device_id_type=MESH,
        )

    def signal(sem, order):
        pl.semaphore_signal(sem, inc=1, device_id=device(order), device_id_type=MESH)

    loads = [
        pltpu.make_async_copy(source, target, load_sem.at[i])
        for i, (source, target) in enumerate(
            (
                (gains_hbm.at[0], held),
                (first_hbm, first_ref),
                (second_hbm, second_ref),
                (facet_dir_hbm, facet_dir_ref),
                (vis_hbm, vis),
            )
        )
    ]
    for load in loads:
        load.start()

    barrier = pltpu.get_barrier_semaphore()

    @pl.when(rank > 0)
    def _():
        with jax.named_scope("chain"):
            pl.semaphore_wait(barrier, 1)

    @pl.when(rank < peers - 1)
    def _():
        signal(barrier, rank + 1)

    def greet(order, carry):
        signal(entered.at[layer], order)
        return carry

    lax.fori_loop(0, rank, greet, 0)

    with jax.named_scope("gains"):
        loads[0].wait()
    lane = lax.broadcasted_iota(jnp.int32, (8, LANES), 1)
    total_slots = peers * slots
    urgent = FREE_LAYERS * pol_count

    def pack(where):
        base = where * slots
        for chan in range(chans):
            for half in range(2):
                outgoing[where, chan * 2 + half] = window(held, chan, (base + 2 * half) * ARRAY_STATIONS)
        last = min(base + slots, total_slots - 1) * ARRAY_STATIONS
        outgoing[where, 2 * chans] = jnp.where(
            lane < LANES // 2, window(held, 0, last), pltpu.roll(window(held, 1, last), LANES // 2, 1)
        )

    def send(order, carry):
        to(order, send_sem).start()
        return carry

    def hasten(order, carry):
        to(order, urgent_sem.at[order]).start()
        return carry

    def hasten_next(order, carry):
        to(order - IN_FLIGHT, urgent_sem.at[order - IN_FLIGHT]).wait_send()
        return hasten(order, carry)

    def hastened(order, carry):
        to(order, urgent_sem.at[order]).wait_send()
        return carry

    free = jnp.clip((layers - layer + 2) // 2, 1, FREE_LAYERS)
    hurry = jnp.minimum(rank, free * pol_count)
    for where in range(IN_FLIGHT + 1):
        pack(where)
    with jax.named_scope("urgent"):
        lax.fori_loop(0, jnp.minimum(rank, IN_FLIGHT), hasten, 0)
        for where in range(IN_FLIGHT + 1, peers):
            pack(where)
        lax.fori_loop(IN_FLIGHT, hurry, hasten_next, 0)
        lax.fori_loop(jnp.maximum(hurry - IN_FLIGHT, 0), hurry, hastened, 0)

    gated = layers - FREE_LAYERS - 1

    def far_from(low):
        return jnp.maximum(low + half + 1, jnp.where(low == 0, layers, jnp.maximum(layers + 1 - 2 * low, gated)))

    above_from = jnp.where(layer < FREE_LAYERS, far_from(layer), jnp.minimum(far_from(layer), gated + 1))
    above_from = jnp.where(layer <= 1, layers, jnp.minimum(jnp.maximum(above_from, layer + 1), layers))
    alone = shifted & (rank == behind)
    far_below = jnp.where((layer < gated) | alone, free, jnp.maximum(layer - half, free))

    def drain():
        paced = jnp.where(layer == layers - 1, (far_below - free) * pol_count, 0)
        paced = jnp.where((layer > 0) & (layer < half), (layers - above_from) * pol_count, paced)
        for count in range(1, peers):

            @pl.when(peers - 1 - hurry - paced == count)
            def _():
                transfers(0, count, send_sem, layer).wait_send()

    def wait_turn():
        with jax.named_scope("go"):
            pl.semaphore_wait(go, 1)

    def send_far():
        @pl.when((layer >= gated) & (layer < layers - 1))
        def _():
            def turn_of(low, carry):
                wait_turn()
                for core in range(pol_count):
                    send(low * pol_count + core, 0)
                return carry

            lax.fori_loop(free, far_below, turn_of, 0)

        @pl.when(layer == layers - 1)
        def _():
            def release(low):
                @pl.when(rank == peers - pol_count)
                def _():
                    def allow(order, carry):
                        signal(go, order)
                        return carry

                    def allow_gated(order, carry):
                        @pl.when(jnp.logical_not(shifted & (order == behind)))
                        def _():
                            signal(go, order)

                        return carry

                    lax.fori_loop(far_from(low) * pol_count, peers - pol_count, allow_gated, 0)

                    @pl.when(low == LAST_GO)
                    def _():
                        lax.fori_loop(half * pol_count, peers - pol_count, allow, 0)

            for low in range(1, 1 + LOOK_AHEAD):
                release(low)

            def turn_of(low, carry):
                release(low + LOOK_AHEAD)
                for core in range(pol_count):
                    to(low * pol_count + core, urgent_sem.at[core]).start()
                for core in range(pol_count):
                    to(low * pol_count + core, urgent_sem.at[core]).wait_send()
                return carry

            lax.fori_loop(free, far_below, turn_of, 0)

    def answer_last():
        @pl.when((layer >= half) & (layer < layers - 1))
        def _():
            wait_turn()
            lax.fori_loop(above_from * pol_count, peers, send, 0)

        @pl.when((layer > 0) & (layer < half))
        def _():
            base = above_from * pol_count

            @pl.when(layer == 1)
            def _():
                drain()

            @pl.when(layer > 1)
            def _():
                wait_turn()

                def start(order, carry):
                    to(order, urgent_sem.at[order - base]).start()
                    return carry

                lax.fori_loop(base, peers, start, 0)

                @pl.when((layer < half - 1) & (layer >= EARLY))
                def _():
                    signal(go, rank + pol_count)

                def wait(order, carry):
                    to(order, urgent_sem.at[order - base]).wait_send()
                    return carry

                with jax.named_scope("left"):
                    lax.fori_loop(base, peers, wait, 0)

            @pl.when((layer < half - 1) & (layer < EARLY))
            def _():
                signal(go, rank + pol_count)

    incoming[rank] = outgoing[place(rank)]
    with jax.named_scope("loads"):
        for load in loads[1:]:
            load.wait()

    unit = lax.broadcasted_iota(jnp.int32, (8, LANES), 0)
    slot_of_unit = lax.rem(unit, slots)
    live = slot_of_unit * LANES + lane < filled_ref[0]
    after = (lane.astype(jnp.float32) + 0.5) / LANES
    before = 1.0 - after

    def spread(where, ref, rows):
        for slot in range(slots):
            station = jnp.broadcast_to(ref[slot : slot + 1, :], (8, LANES))
            upper = station + ARRAY_STATIONS
            for chan in range(chans):
                now = incoming[where, chan * 2 + slot // 2]
                if slot % 2 == 0:
                    low, high = gather_lanes(now, station), gather_lanes(now, upper)
                else:
                    low = gather_lanes(now, upper)
                    if slot + 1 < slots:
                        high = gather_lanes(incoming[where, chan * 2 + slot // 2 + 1], station)
                    else:
                        high = gather_lanes(incoming[where, 2 * chans], station + chan * (LANES // 2))
                at = (chan * slots + slot) * 8
                rows[at : at + 8, :] = before * low + after * high

    def component(rows, k):
        return rows[pl.ds(k, 8, stride=8), :]

    def correct(order, where):
        spread(order, first_ref, left_rows)
        spread(order, second_ref, right_rows)
        left = [component(left_rows, k) for k in range(8)]
        right = [component(right_rows, k) for k in range(8)]
        data = [component(data_rows, k) for k in range(8)]
        for row in (0, 1):
            half_re, half_im = [], []
            for column in (0, 1):
                re = im = None
                for middle in (0, 1):
                    l_re, l_im = left[2 * row + middle], left[4 + 2 * row + middle]
                    d_re, d_im = data[2 * middle + column], data[4 + 2 * middle + column]
                    p_re = l_re * d_re - l_im * d_im
                    p_im = l_re * d_im + l_im * d_re
                    re = p_re if re is None else re + p_re
                    im = p_im if im is None else im + p_im
                half_re.append(re)
                half_im.append(im)
            for out in (0, 1):
                re = im = None
                for column in (0, 1):
                    r_re, r_im = right[2 * out + column], right[4 + 2 * out + column]
                    p_re = half_re[column] * r_re + half_im[column] * r_im
                    p_im = half_im[column] * r_re - half_re[column] * r_im
                    re = p_re if re is None else re + p_re
                    im = p_im if im is None else im + p_im
                out_rows[pl.ds(2 * row + out, 8, stride=8), :] = jnp.where(live, re, 0.0)
                out_rows[pl.ds(4 + 2 * row + out, 8, stride=8), :] = jnp.where(live, im, 0.0)
        for chan in range(chans):
            for slot in range(slots):
                at = (chan * slots + slot) * 8
                done[where, chan, :, slot * LANES : (slot + 1) * LANES] = out_rows[at : at + 8, :].astype(done.dtype)

    def take(order):
        where = place(order)
        facet = jnp.int32(0)
        for f in range(peers):
            facet = jnp.where(facet_dir_ref[f] == where, f, facet)
        for chan in range(chans):
            for slot in range(slots):
                at = (chan * slots + slot) * 8
                data_rows[at : at + 8, :] = vis[facet, chan, :, slot * LANES : (slot + 1) * LANES].astype(jnp.float32)
        correct(order, where)

    above = layers - 1 - layer
    near_above = above_from - 1 - layer

    last_step = jnp.where(layer <= 1, layers - 3, near_above + 1 + jnp.where(layer < half, layer, 0))
    last_turn = jnp.maximum(above, jnp.minimum(last_step, layers - 1) + LAG)

    def answer(turn, carry):
        @pl.when((turn == 0) & (rank < partner))
        def _():
            pl.semaphore_wait(entered.at[layer], pol_count - 1)
            send(partner, 0)

        @pl.when((turn == 0) & (rank > partner) & (layer >= free))
        def _():
            send(partner, 0)

        @pl.when((turn > 0) & (turn <= above))
        def _():
            with jax.named_scope("hello"):
                pl.semaphore_wait(entered.at[layer + turn], pol_count)

            @pl.when(layer + turn < above_from)
            def _():
                for core in range(pol_count):
                    send((layer + turn) * pol_count + core, 0)

        first = jnp.where(turn == 0, far_below, far_below + turn + 1)
        last = jnp.where(turn < above, jnp.minimum(far_below + turn + 2, layer), jnp.where(turn == above, layer, 0))

        def send_near(low, carry):
            for core in range(pol_count):
                send(low * pol_count + core, 0)
            return carry

        @pl.when(layer < layers - 1)
        def _():
            lax.fori_loop(first, last, send_near, 0)

        @pl.when(turn == above)
        def _():
            send_far()

        @pl.when(layer == layers - 1)
        def _():
            lax.fori_loop(first, last, send_near, 0)

        step = turn - LAG

        @pl.when(turn == last_turn)
        def _():
            answer_last()

        @pl.when(step == 0)
        def _():
            take(rank)
            transfers(partner, pol_count - 1, send_sem, layer).wait_recv()
            take(partner)

        @pl.when(step > 0)
        def _():
            source = jnp.where(step <= near_above, layer + step, step)
            source = jnp.where((step > near_above) & (step <= near_above + layer), step - near_above - 1, source)
            with jax.named_scope("arrive"):
                transfers(source * pol_count, pol_count, send_sem, source).wait_recv()
            with jax.named_scope("correct"):

                def both(core, carry):
                    take(source * pol_count + core)
                    return carry

                lax.fori_loop(0, pol_count, both, 0)

        return carry

    lax.fori_loop(0, layers + LAG, answer, 0)

    with jax.named_scope("finish"):

        @pl.when(layer != 1)
        def _():
            drain()

    with jax.named_scope("order"):
        for f in range(peers):
            out_ref[f] = done[facet_dir_ref[f]]


def shards(gains, visibilities, first_station, second_station, filled_row_count, facet_dir):
    bt_count, pol_count = lax.axis_size("bt"), lax.axis_size("pol")
    peers = bt_count * pol_count
    chans = gains.shape[1]
    hbm = pl.BlockSpec(memory_space=pltpu.HBM)
    vmem = pl.BlockSpec(memory_space=pltpu.VMEM)
    rows = 8 * chans * GAIN_SLOT_COUNT
    operands = (
        facet_dir,
        first_station.reshape(GAIN_SLOT_COUNT, LANES),
        second_station.reshape(GAIN_SLOT_COUNT, LANES),
        gains,
        visibilities,
    )
    return pl.pallas_call(
        functools.partial(kernel, peers, bt_count, pol_count),
        name="correct",
        out_shape=jax.ShapeDtypeStruct(visibilities.shape, visibilities.dtype),
        in_specs=[pl.BlockSpec(memory_space=pltpu.SMEM)] + [hbm] * 5,
        out_specs=vmem,
        scratch_shapes=[
            pltpu.SMEM(facet_dir.shape, jnp.int32),
            pltpu.VMEM((GAIN_SLOT_COUNT, LANES), jnp.int32),
            pltpu.VMEM((GAIN_SLOT_COUNT, LANES), jnp.int32),
            pltpu.VMEM(gains.shape[1:], jnp.float32),
            pltpu.VMEM((peers, TILES, 8, LANES), jnp.float32),
            pltpu.VMEM((peers, TILES, 8, LANES), jnp.float32),
            pltpu.VMEM(visibilities.shape, visibilities.dtype),
            pltpu.VMEM(visibilities.shape, visibilities.dtype),
            pltpu.VMEM((rows, LANES), jnp.float32),
            pltpu.VMEM((rows, LANES), jnp.float32),
            pltpu.VMEM((rows, LANES), jnp.float32),
            pltpu.VMEM((rows, LANES), jnp.float32),
            pltpu.SemaphoreType.DMA((5,)),
            pltpu.SemaphoreType.DMA(((FREE_LAYERS + 1) * pol_count,)),
            pltpu.SemaphoreType.DMA,
            pltpu.SemaphoreType.DMA((bt_count,)),
            pltpu.SemaphoreType.REGULAR((bt_count,)),
            pltpu.SemaphoreType.REGULAR,
        ],
        compiler_params=pltpu.CompilerParams(collective_id=0, has_side_effects=True, vmem_limit_bytes=8 << 20),
    )(filled_row_count, *(pltpu.with_memory_space_constraint(x, pltpu.HBM) for x in operands))


def solution(mesh):
    return jax.shard_map(
        shards,
        mesh=mesh,
        in_specs=(
            P(("obs", "bt", "pol"), "freq", None, None),
            P("obs", "freq", None, ("bt", "pol")),
            P(("obs", "bt", "pol")),
            P(("obs", "bt", "pol")),
            P(("obs", "bt", "pol")),
            P("obs"),
        ),
        out_specs=P("obs", "freq", None, ("bt", "pol")),
        check_vma=False,
    )
```

```python
import functools

import jax
import jax.numpy as jnp
from jax import lax
from jax.experimental import pallas as pl
from jax.experimental.pallas import tpu as pltpu
from jax.sharding import PartitionSpec as P

ARRAY_STATIONS = 62
GAIN_SLOT_COUNT = 4
LANES = 128
TILES = 5
IN_FLIGHT = 2
FREE_LAYERS = 3
LAG = 4
LAST_GO = 6
LOOK_AHEAD = 1
EARLY = 5
MESH = pl.DeviceIdType.MESH


def gather_lanes(tile, index):
    return jnp.take_along_axis(tile, index, axis=1, mode="promise_in_bounds")


def window(held, chan, start):
    tile, shift = divmod(start, LANES)
    here = held[chan, :, tile * LANES : (tile + 1) * LANES]
    if shift == 0:
        return here
    lane = lax.broadcasted_iota(jnp.int32, here.shape, 1)
    if (tile + 1) * LANES < held.shape[2]:
        after = held[chan, :, (tile + 1) * LANES : (tile + 2) * LANES]
        here = jnp.where(lane >= shift, here, after)
    return pltpu.roll(here, LANES - shift, 1)


def kernel(
    peers,
    bt_count,
    pol_count,
    filled_ref,
    facet_dir_hbm,
    first_hbm,
    second_hbm,
    gains_hbm,
    vis_hbm,
    out_ref,
    facet_dir_ref,
    first_ref,
    second_ref,
    held,
    outgoing,
    incoming,
    vis,
    done,
    left_rows,
    right_rows,
    data_rows,
    out_rows,
    load_sem,
    urgent_sem,
    send_sem,
    recv_sem,
    entered,
    go,
):
    chans = held.shape[0]
    slots = GAIN_SLOT_COUNT
    layers, half = peers // pol_count, bt_count // 2
    own_place = lax.axis_index("bt") * pol_count + lax.axis_index("pol")
    behind = (layers - 2) * pol_count - 1
    shifted = (lax.axis_index("obs") == 0) & (lax.axis_index("freq") == 0)
    rank = jnp.where(own_place == 0, behind, jnp.where(own_place <= behind, own_place - 1, own_place))
    rank = jnp.where(shifted, rank, own_place)
    layer = rank // pol_count
    partner = layer * pol_count + lax.rem(rank + 1, pol_count)

    def place(order):
        moved = jnp.where(order == behind, 0, jnp.where(order < behind, order + 1, order))
        return jnp.where(shifted, moved, order)

    def device(order):
        where = place(order)
        return {"bt": where // pol_count, "pol": lax.rem(where, pol_count)}

    def to(order, sem):
        return pltpu.make_async_remote_copy(
            src_ref=outgoing.at[place(order)],
            dst_ref=incoming.at[rank],
            send_sem=sem,
            recv_sem=recv_sem.at[layer],
            device_id=device(order),
            device_id_type=MESH,
        )

    def transfers(start, count, sem, into):
        return pltpu.make_async_remote_copy(
            src_ref=outgoing.at[pl.ds(start, count)],
            dst_ref=incoming.at[pl.ds(start, count)],
            send_sem=sem,
            recv_sem=recv_sem.at[into],
            device_id=device(partner),
            device_id_type=MESH,
        )

    def signal(sem, order):
        pl.semaphore_signal(sem, inc=1, device_id=device(order), device_id_type=MESH)

    loads = [
        pltpu.make_async_copy(source, target, load_sem.at[i])
        for i, (source, target) in enumerate(
            (
                (gains_hbm.at[0], held),
                (first_hbm, first_ref),
                (second_hbm, second_ref),
                (facet_dir_hbm, facet_dir_ref),
                (vis_hbm, vis),
            )
        )
    ]
    for load in loads:
        load.start()

    barrier = pltpu.get_barrier_semaphore()

    @pl.when(rank > 0)
    def _():
        with jax.named_scope("chain"):
            pl.semaphore_wait(barrier, 1)

    @pl.when(rank < peers - 1)
    def _():
        signal(barrier, rank + 1)

    def greet(order, carry):
        signal(entered.at[layer], order)
        return carry

    lax.fori_loop(0, rank, greet, 0)

    with jax.named_scope("gains"):
        loads[0].wait()
    lane = lax.broadcasted_iota(jnp.int32, (8, LANES), 1)
    total_slots = peers * slots
    urgent = FREE_LAYERS * pol_count

    def pack(where):
        base = where * slots
        for chan in range(chans):
            for half in range(2):
                outgoing[where, chan * 2 + half] = window(held, chan, (base + 2 * half) * ARRAY_STATIONS)
        last = min(base + slots, total_slots - 1) * ARRAY_STATIONS
        outgoing[where, 2 * chans] = jnp.where(
            lane < LANES // 2, window(held, 0, last), pltpu.roll(window(held, 1, last), LANES // 2, 1)
        )

    def send(order, carry):
        to(order, send_sem).start()
        return carry

    def hasten(order, carry):
        to(order, urgent_sem.at[order]).start()
        return carry

    def hasten_next(order, carry):
        to(order - IN_FLIGHT, urgent_sem.at[order - IN_FLIGHT]).wait_send()
        return hasten(order, carry)

    def hastened(order, carry):
        to(order, urgent_sem.at[order]).wait_send()
        return carry

    free = jnp.clip(layers - layer, 1, FREE_LAYERS)
    hurry = jnp.minimum(rank, free * pol_count)
    for where in range(IN_FLIGHT + 1):
        pack(where)
    with jax.named_scope("urgent"):
        lax.fori_loop(0, jnp.minimum(rank, IN_FLIGHT), hasten, 0)
        for where in range(IN_FLIGHT + 1, peers):
            pack(where)
        lax.fori_loop(IN_FLIGHT, hurry, hasten_next, 0)
        lax.fori_loop(jnp.maximum(hurry - IN_FLIGHT, 0), hurry, hastened, 0)

    gated = layers - FREE_LAYERS - 1

    def far_from(low):
        return jnp.maximum(low + half + 1, jnp.where(low == 0, layers, jnp.where(low < FREE_LAYERS, layers - low, gated)))

    above_from = jnp.where(layer < FREE_LAYERS, far_from(layer), jnp.minimum(far_from(layer), gated + 1))
    above_from = jnp.where(layer <= 1, layers, jnp.minimum(jnp.maximum(above_from, layer + 1), layers))
    alone = shifted & (rank == behind)
    far_below = jnp.where((layer < gated) | alone, free, jnp.maximum(layer - half, free))

    def drain():
        paced = jnp.where(layer == layers - 1, (far_below - free) * pol_count, 0)
        paced = jnp.where((layer > 0) & (layer < half), (layers - above_from) * pol_count, paced)
        for count in range(1, peers):

            @pl.when(peers - 1 - hurry - paced == count)
            def _():
                transfers(0, count, send_sem, layer).wait_send()

    def wait_turn():
        with jax.named_scope("go"):
            pl.semaphore_wait(go, 1)

    def send_far():
        @pl.when((layer >= gated) & (layer < layers - 1))
        def _():
            def turn_of(low, carry):
                wait_turn()
                for core in range(pol_count):
                    send(low * pol_count + core, 0)
                return carry

            lax.fori_loop(free, far_below, turn_of, 0)

        @pl.when(layer == layers - 1)
        def _():
            def release(low):
                @pl.when(rank == peers - pol_count)
                def _():
                    def allow(order, carry):
                        signal(go, order)
                        return carry

                    def allow_gated(order, carry):
                        @pl.when(jnp.logical_not(shifted & (order == behind)))
                        def _():
                            signal(go, order)

                        return carry

                    lax.fori_loop(far_from(low) * pol_count, peers - pol_count, allow_gated, 0)

                    @pl.when(low == LAST_GO)
                    def _():
                        lax.fori_loop(half * pol_count, peers - pol_count, allow, 0)

            for low in range(1, 1 + LOOK_AHEAD):
                release(low)

            def turn_of(low, carry):
                release(low + LOOK_AHEAD)
                for core in range(pol_count):
                    to(low * pol_count + core, urgent_sem.at[core]).start()
                for core in range(pol_count):
                    to(low * pol_count + core, urgent_sem.at[core]).wait_send()
                return carry

            lax.fori_loop(free, far_below, turn_of, 0)

    def answers_left():
        base = above_from * pol_count

        def wait(order, carry):
            to(order, urgent_sem.at[order - base]).wait_send()
            return carry

        with jax.named_scope("left"):
            lax.fori_loop(base, peers, wait, 0)

    def answer_last():
        @pl.when((layer >= half) & (layer < layers - 1))
        def _():
            wait_turn()
            lax.fori_loop(above_from * pol_count, peers, send, 0)

        @pl.when((layer > 0) & (layer < half))
        def _():
            base = above_from * pol_count

            @pl.when(layer == 1)
            def _():
                drain()

            @pl.when(layer > 1)
            def _():
                wait_turn()

                def start(order, carry):
                    to(order, urgent_sem.at[order - base]).start()
                    return carry

                lax.fori_loop(base, peers, start, 0)

                @pl.when((layer < half - 1) & (layer >= EARLY))
                def _():
                    signal(go, rank + pol_count)

                @pl.when(layer < EARLY)
                def _():
                    answers_left()

            @pl.when((layer < half - 1) & (layer < EARLY))
            def _():
                signal(go, rank + pol_count)

    incoming[rank] = outgoing[place(rank)]
    with jax.named_scope("loads"):
        for load in loads[1:]:
            load.wait()

    unit = lax.broadcasted_iota(jnp.int32, (8, LANES), 0)
    slot_of_unit = lax.rem(unit, slots)
    live = slot_of_unit * LANES + lane < filled_ref[0]
    after = (lane.astype(jnp.float32) + 0.5) / LANES
    before = 1.0 - after

    def spread(where, ref, rows):
        for slot in range(slots):
            station = jnp.broadcast_to(ref[slot : slot + 1, :], (8, LANES))
            upper = station + ARRAY_STATIONS
            for chan in range(chans):
                now = incoming[where, chan * 2 + slot // 2]
                if slot % 2 == 0:
                    low, high = gather_lanes(now, station), gather_lanes(now, upper)
                else:
                    low = gather_lanes(now, upper)
                    if slot + 1 < slots:
                        high = gather_lanes(incoming[where, chan * 2 + slot // 2 + 1], station)
                    else:
                        high = gather_lanes(incoming[where, 2 * chans], station + chan * (LANES // 2))
                at = (chan * slots + slot) * 8
                rows[at : at + 8, :] = before * low + after * high

    def component(rows, k):
        return rows[pl.ds(k, 8, stride=8), :]

    def correct(order, where):
        spread(order, first_ref, left_rows)
        spread(order, second_ref, right_rows)
        left = [component(left_rows, k) for k in range(8)]
        right = [component(right_rows, k) for k in range(8)]
        data = [component(data_rows, k) for k in range(8)]
        for row in (0, 1):
            half_re, half_im = [], []
            for column in (0, 1):
                re = im = None
                for middle in (0, 1):
                    l_re, l_im = left[2 * row + middle], left[4 + 2 * row + middle]
                    d_re, d_im = data[2 * middle + column], data[4 + 2 * middle + column]
                    p_re = l_re * d_re - l_im * d_im
                    p_im = l_re * d_im + l_im * d_re
                    re = p_re if re is None else re + p_re
                    im = p_im if im is None else im + p_im
                half_re.append(re)
                half_im.append(im)
            for out in (0, 1):
                re = im = None
                for column in (0, 1):
                    r_re, r_im = right[2 * out + column], right[4 + 2 * out + column]
                    p_re = half_re[column] * r_re + half_im[column] * r_im
                    p_im = half_im[column] * r_re - half_re[column] * r_im
                    re = p_re if re is None else re + p_re
                    im = p_im if im is None else im + p_im
                out_rows[pl.ds(2 * row + out, 8, stride=8), :] = jnp.where(live, re, 0.0)
                out_rows[pl.ds(4 + 2 * row + out, 8, stride=8), :] = jnp.where(live, im, 0.0)
        for chan in range(chans):
            for slot in range(slots):
                at = (chan * slots + slot) * 8
                done[where, chan, :, slot * LANES : (slot + 1) * LANES] = out_rows[at : at + 8, :].astype(done.dtype)

    def take(order):
        where = place(order)
        facet = jnp.int32(0)
        for f in range(peers):
            facet = jnp.where(facet_dir_ref[f] == where, f, facet)
        for chan in range(chans):
            for slot in range(slots):
                at = (chan * slots + slot) * 8
                data_rows[at : at + 8, :] = vis[facet, chan, :, slot * LANES : (slot + 1) * LANES].astype(jnp.float32)
        correct(order, where)

    above = layers - 1 - layer
    near_above = above_from - 1 - layer

    last_step = jnp.where(layer <= 1, layers - 3, near_above + 1 + jnp.where(layer < half, layer, 0))
    last_turn = jnp.maximum(above, jnp.minimum(last_step, layers - 1) + LAG)

    def answer(turn, carry):
        @pl.when((turn == 0) & (rank < partner))
        def _():
            pl.semaphore_wait(entered.at[layer], pol_count - 1)
            send(partner, 0)

        @pl.when((turn == 0) & (rank > partner) & (layer >= free))
        def _():
            send(partner, 0)

        @pl.when((turn > 0) & (turn <= above))
        def _():
            with jax.named_scope("hello"):
                pl.semaphore_wait(entered.at[layer + turn], pol_count)

            @pl.when(layer + turn < above_from)
            def _():
                for core in range(pol_count):
                    send((layer + turn) * pol_count + core, 0)

        first = jnp.where(turn == 0, far_below, far_below + turn + 1)
        last = jnp.where(turn < above, jnp.minimum(far_below + turn + 2, layer), jnp.where(turn == above, layer, 0))

        def send_near(low, carry):
            for core in range(pol_count):
                send(low * pol_count + core, 0)
            return carry

        @pl.when(layer < layers - 1)
        def _():
            lax.fori_loop(first, last, send_near, 0)

        @pl.when(turn == above)
        def _():
            send_far()

        @pl.when(layer == layers - 1)
        def _():
            lax.fori_loop(first, last, send_near, 0)

        step = turn - LAG

        @pl.when(turn == last_turn)
        def _():
            answer_last()

        @pl.when(step == 0)
        def _():
            take(rank)
            transfers(partner, pol_count - 1, send_sem, layer).wait_recv()
            take(partner)

        @pl.when(step > 0)
        def _():
            source = jnp.where(step <= near_above, layer + step, step)
            source = jnp.where((step > near_above) & (step <= near_above + layer), step - near_above - 1, source)
            with jax.named_scope("arrive"):
                transfers(source * pol_count, pol_count, send_sem, source).wait_recv()
            with jax.named_scope("correct"):

                def both(core, carry):
                    take(source * pol_count + core)
                    return carry

                lax.fori_loop(0, pol_count, both, 0)

        return carry

    lax.fori_loop(0, layers + LAG, answer, 0)

    with jax.named_scope("finish"):

        @pl.when((layer >= EARLY) & (layer < half))
        def _():
            answers_left()

        @pl.when(layer != 1)
        def _():
            drain()

    with jax.named_scope("order"):
        for f in range(peers):
            out_ref[f] = done[facet_dir_ref[f]]


def shards(gains, visibilities, first_station, second_station, filled_row_count, facet_dir):
    bt_count, pol_count = lax.axis_size("bt"), lax.axis_size("pol")
    peers = bt_count * pol_count
    chans = gains.shape[1]
    hbm = pl.BlockSpec(memory_space=pltpu.HBM)
    vmem = pl.BlockSpec(memory_space=pltpu.VMEM)
    rows = 8 * chans * GAIN_SLOT_COUNT
    operands = (
        facet_dir,
        first_station.reshape(GAIN_SLOT_COUNT, LANES),
        second_station.reshape(GAIN_SLOT_COUNT, LANES),
        gains,
        visibilities,
    )
    return pl.pallas_call(
        functools.partial(kernel, peers, bt_count, pol_count),
        name="correct",
        out_shape=jax.ShapeDtypeStruct(visibilities.shape, visibilities.dtype),
        in_specs=[pl.BlockSpec(memory_space=pltpu.SMEM)] + [hbm] * 5,
        out_specs=vmem,
        scratch_shapes=[
            pltpu.SMEM(facet_dir.shape, jnp.int32),
            pltpu.VMEM((GAIN_SLOT_COUNT, LANES), jnp.int32),
            pltpu.VMEM((GAIN_SLOT_COUNT, LANES), jnp.int32),
            pltpu.VMEM(gains.shape[1:], jnp.float32),
            pltpu.VMEM((peers, TILES, 8, LANES), jnp.float32),
            pltpu.VMEM((peers, TILES, 8, LANES), jnp.float32),
            pltpu.VMEM(visibilities.shape, visibilities.dtype),
            pltpu.VMEM(visibilities.shape, visibilities.dtype),
            pltpu.VMEM((rows, LANES), jnp.float32),
            pltpu.VMEM((rows, LANES), jnp.float32),
            pltpu.VMEM((rows, LANES), jnp.float32),
            pltpu.VMEM((rows, LANES), jnp.float32),
            pltpu.SemaphoreType.DMA((5,)),
            pltpu.SemaphoreType.DMA(((FREE_LAYERS + 1) * pol_count,)),
            pltpu.SemaphoreType.DMA,
            pltpu.SemaphoreType.DMA((bt_count,)),
            pltpu.SemaphoreType.REGULAR((bt_count,)),
            pltpu.SemaphoreType.REGULAR,
        ],
        compiler_params=pltpu.CompilerParams(collective_id=0, has_side_effects=True, vmem_limit_bytes=8 << 20),
    )(filled_row_count, *(pltpu.with_memory_space_constraint(x, pltpu.HBM) for x in operands))


def solution(mesh):
    return jax.shard_map(
        shards,
        mesh=mesh,
        in_specs=(
            P(("obs", "bt", "pol"), "freq", None, None),
            P("obs", "freq", None, ("bt", "pol")),
            P(("obs", "bt", "pol")),
            P(("obs", "bt", "pol")),
            P(("obs", "bt", "pol")),
            P("obs"),
        ),
        out_specs=P("obs", "freq", None, ("bt", "pol")),
        check_vma=False,
    )
```

```python
import functools

import jax
import jax.numpy as jnp
from jax import lax
from jax.experimental import pallas as pl
from jax.experimental.pallas import tpu as pltpu
from jax.sharding import PartitionSpec as P

ARRAY_STATIONS = 62
GAIN_SLOT_COUNT = 4
LANES = 128
TILES = 5
IN_FLIGHT = 3
FREE_LAYERS = 3
LAG = 4
LAST_GO = 6
LOOK_AHEAD = 1
EARLY = 5
MESH = pl.DeviceIdType.MESH


def gather_lanes(tile, index):
    return jnp.take_along_axis(tile, index, axis=1, mode="promise_in_bounds")


def window(held, chan, start):
    tile, shift = divmod(start, LANES)
    here = held[chan, :, tile * LANES : (tile + 1) * LANES]
    if shift == 0:
        return here
    lane = lax.broadcasted_iota(jnp.int32, here.shape, 1)
    if (tile + 1) * LANES < held.shape[2]:
        after = held[chan, :, (tile + 1) * LANES : (tile + 2) * LANES]
        here = jnp.where(lane >= shift, here, after)
    return pltpu.roll(here, LANES - shift, 1)


def kernel(
    peers,
    bt_count,
    pol_count,
    filled_ref,
    facet_dir_hbm,
    first_hbm,
    second_hbm,
    gains_hbm,
    vis_hbm,
    out_ref,
    facet_dir_ref,
    first_ref,
    second_ref,
    held,
    outgoing,
    incoming,
    vis,
    done,
    left_rows,
    right_rows,
    data_rows,
    out_rows,
    load_sem,
    urgent_sem,
    send_sem,
    recv_sem,
    entered,
    go,
):
    chans = held.shape[0]
    slots = GAIN_SLOT_COUNT
    layers, half = peers // pol_count, bt_count // 2
    own_place = lax.axis_index("bt") * pol_count + lax.axis_index("pol")
    behind = (layers - 2) * pol_count - 1
    shifted = (lax.axis_index("obs") == 0) & (lax.axis_index("freq") == 0)
    rank = jnp.where(own_place == 0, behind, jnp.where(own_place <= behind, own_place - 1, own_place))
    rank = jnp.where(shifted, rank, own_place)
    layer = rank // pol_count
    partner = layer * pol_count + lax.rem(rank + 1, pol_count)

    def place(order):
        moved = jnp.where(order == behind, 0, jnp.where(order < behind, order + 1, order))
        return jnp.where(shifted, moved, order)

    def device(order):
        where = place(order)
        return {"bt": where // pol_count, "pol": lax.rem(where, pol_count)}

    def to(order, sem):
        return pltpu.make_async_remote_copy(
            src_ref=outgoing.at[place(order)],
            dst_ref=incoming.at[rank],
            send_sem=sem,
            recv_sem=recv_sem.at[layer],
            device_id=device(order),
            device_id_type=MESH,
        )

    def transfers(start, count, sem, into):
        return pltpu.make_async_remote_copy(
            src_ref=outgoing.at[pl.ds(start, count)],
            dst_ref=incoming.at[pl.ds(start, count)],
            send_sem=sem,
            recv_sem=recv_sem.at[into],
            device_id=device(partner),
            device_id_type=MESH,
        )

    def signal(sem, order):
        pl.semaphore_signal(sem, inc=1, device_id=device(order), device_id_type=MESH)

    loads = [
        pltpu.make_async_copy(source, target, load_sem.at[i])
        for i, (source, target) in enumerate(
            (
                (gains_hbm.at[0], held),
                (first_hbm, first_ref),
                (second_hbm, second_ref),
                (facet_dir_hbm, facet_dir_ref),
                (vis_hbm, vis),
            )
        )
    ]
    for load in loads:
        load.start()

    barrier = pltpu.get_barrier_semaphore()

    @pl.when(rank > 0)
    def _():
        with jax.named_scope("chain"):
            pl.semaphore_wait(barrier, 1)

    @pl.when(rank < peers - 1)
    def _():
        signal(barrier, rank + 1)

    def greet(order, carry):
        signal(entered.at[layer], order)
        return carry

    lax.fori_loop(0, rank, greet, 0)

    with jax.named_scope("gains"):
        loads[0].wait()
    lane = lax.broadcasted_iota(jnp.int32, (8, LANES), 1)
    total_slots = peers * slots
    urgent = FREE_LAYERS * pol_count

    def pack(where):
        base = where * slots
        for chan in range(chans):
            for half in range(2):
                outgoing[where, chan * 2 + half] = window(held, chan, (base + 2 * half) * ARRAY_STATIONS)
        last = min(base + slots, total_slots - 1) * ARRAY_STATIONS
        outgoing[where, 2 * chans] = jnp.where(
            lane < LANES // 2, window(held, 0, last), pltpu.roll(window(held, 1, last), LANES // 2, 1)
        )

    def send(order, carry):
        to(order, send_sem).start()
        return carry

    def hasten(order, carry):
        to(order, urgent_sem.at[order]).start()
        return carry

    def hasten_next(order, carry):
        to(order - IN_FLIGHT, urgent_sem.at[order - IN_FLIGHT]).wait_send()
        return hasten(order, carry)

    def hastened(order, carry):
        to(order, urgent_sem.at[order]).wait_send()
        return carry

    free = jnp.clip(layers - layer, 1, FREE_LAYERS)
    hurry = jnp.minimum(rank, free * pol_count)
    for where in range(IN_FLIGHT + 1):
        pack(where)
    with jax.named_scope("urgent"):
        lax.fori_loop(0, jnp.minimum(hurry, IN_FLIGHT), hasten, 0)
        for where in range(IN_FLIGHT + 1, peers):
            pack(where)
        lax.fori_loop(IN_FLIGHT, hurry, hasten_next, 0)
        lax.fori_loop(jnp.maximum(hurry - IN_FLIGHT, 0), hurry, hastened, 0)

    gated = layers - FREE_LAYERS - 1

    def far_from(low):
        return jnp.maximum(low + half + 1, jnp.where(low == 0, layers, jnp.where(low < FREE_LAYERS, layers - low, gated)))

    above_from = jnp.where(layer < FREE_LAYERS, far_from(layer), jnp.minimum(far_from(layer), gated + 1))
    above_from = jnp.where(layer <= 1, layers, jnp.minimum(jnp.maximum(above_from, layer + 1), layers))
    alone = shifted & (rank == behind)
    far_below = jnp.where((layer < gated) | alone, free, jnp.maximum(layer - half, free))

    def drain():
        paced = jnp.where(layer == layers - 1, (far_below - free) * pol_count, 0)
        paced = jnp.where((layer > 0) & (layer < half), (layers - above_from) * pol_count, paced)
        for count in range(1, peers):

            @pl.when(peers - 1 - hurry - paced == count)
            def _():
                transfers(0, count, send_sem, layer).wait_send()

    def wait_turn():
        with jax.named_scope("go"):
            pl.semaphore_wait(go, 1)

    def send_far():
        @pl.when((layer >= gated) & (layer < layers - 1))
        def _():
            def turn_of(low, carry):
                wait_turn()
                for core in range(pol_count):
                    send(low * pol_count + core, 0)
                return carry

            lax.fori_loop(free, far_below, turn_of, 0)

        @pl.when(layer == layers - 1)
        def _():
            def release(low):
                @pl.when(rank == peers - pol_count)
                def _():
                    def allow(order, carry):
                        signal(go, order)
                        return carry

                    def allow_gated(order, carry):
                        @pl.when(jnp.logical_not(shifted & (order == behind)))
                        def _():
                            signal(go, order)

                        return carry

                    lax.fori_loop(far_from(low) * pol_count, peers - pol_count, allow_gated, 0)

                    @pl.when(low == LAST_GO)
                    def _():
                        lax.fori_loop(half * pol_count, peers - pol_count, allow, 0)

            for low in range(1, 1 + LOOK_AHEAD):
                release(low)

            def turn_of(low, carry):
                release(low + LOOK_AHEAD)
                for core in range(pol_count):
                    to(low * pol_count + core, urgent_sem.at[core]).start()
                for core in range(pol_count):
                    to(low * pol_count + core, urgent_sem.at[core]).wait_send()
                return carry

            lax.fori_loop(free, far_below, turn_of, 0)

    def answers_left():
        base = above_from * pol_count

        def wait(order, carry):
            to(order, urgent_sem.at[order - base]).wait_send()
            return carry

        with jax.named_scope("left"):
            lax.fori_loop(base, peers, wait, 0)

    def answer_last():
        @pl.when((layer >= half) & (layer < layers - 1))
        def _():
            wait_turn()
            lax.fori_loop(above_from * pol_count, peers, send, 0)

        @pl.when((layer > 0) & (layer < half))
        def _():
            base = above_from * pol_count

            @pl.when(layer == 1)
            def _():
                drain()

            @pl.when(layer > 1)
            def _():
                wait_turn()

                def start(order, carry):
                    to(order, urgent_sem.at[order - base]).start()
                    return carry

                lax.fori_loop(base, peers, start, 0)

                @pl.when((layer < half - 1) & (layer >= EARLY))
                def _():
                    signal(go, rank + pol_count)

                @pl.when(layer < EARLY)
                def _():
                    answers_left()

            @pl.when((layer < half - 1) & (layer < EARLY))
            def _():
                signal(go, rank + pol_count)

    incoming[rank] = outgoing[place(rank)]
    with jax.named_scope("loads"):
        for load in loads[1:]:
            load.wait()

    unit = lax.broadcasted_iota(jnp.int32, (8, LANES), 0)
    slot_of_unit = lax.rem(unit, slots)
    live = slot_of_unit * LANES + lane < filled_ref[0]
    after = (lane.astype(jnp.float32) + 0.5) / LANES
    before = 1.0 - after

    def spread(where, ref, rows):
        for slot in range(slots):
            station = jnp.broadcast_to(ref[slot : slot + 1, :], (8, LANES))
            upper = station + ARRAY_STATIONS
            for chan in range(chans):
                now = incoming[where, chan * 2 + slot // 2]
                if slot % 2 == 0:
                    low, high = gather_lanes(now, station), gather_lanes(now, upper)
                else:
                    low = gather_lanes(now, upper)
                    if slot + 1 < slots:
                        high = gather_lanes(incoming[where, chan * 2 + slot // 2 + 1], station)
                    else:
                        high = gather_lanes(incoming[where, 2 * chans], station + chan * (LANES // 2))
                at = (chan * slots + slot) * 8
                rows[at : at + 8, :] = before * low + after * high

    def component(rows, k):
        return rows[pl.ds(k, 8, stride=8), :]

    def correct(order, where):
        spread(order, first_ref, left_rows)
        spread(order, second_ref, right_rows)
        left = [component(left_rows, k) for k in range(8)]
        right = [component(right_rows, k) for k in range(8)]
        data = [component(data_rows, k) for k in range(8)]
        for row in (0, 1):
            half_re, half_im = [], []
            for column in (0, 1):
                re = im = None
                for middle in (0, 1):
                    l_re, l_im = left[2 * row + middle], left[4 + 2 * row + middle]
                    d_re, d_im = data[2 * middle + column], data[4 + 2 * middle + column]
                    p_re = l_re * d_re - l_im * d_im
                    p_im = l_re * d_im + l_im * d_re
                    re = p_re if re is None else re + p_re
                    im = p_im if im is None else im + p_im
                half_re.append(re)
                half_im.append(im)
            for out in (0, 1):
                re = im = None
                for column in (0, 1):
                    r_re, r_im = right[2 * out + column], right[4 + 2 * out + column]
                    p_re = half_re[column] * r_re + half_im[column] * r_im
                    p_im = half_im[column] * r_re - half_re[column] * r_im
                    re = p_re if re is None else re + p_re
                    im = p_im if im is None else im + p_im
                out_rows[pl.ds(2 * row + out, 8, stride=8), :] = jnp.where(live, re, 0.0)
                out_rows[pl.ds(4 + 2 * row + out, 8, stride=8), :] = jnp.where(live, im, 0.0)
        for chan in range(chans):
            for slot in range(slots):
                at = (chan * slots + slot) * 8
                done[where, chan, :, slot * LANES : (slot + 1) * LANES] = out_rows[at : at + 8, :].astype(done.dtype)

    def take(order):
        where = place(order)
        facet = jnp.int32(0)
        for f in range(peers):
            facet = jnp.where(facet_dir_ref[f] == where, f, facet)
        for chan in range(chans):
            for slot in range(slots):
                at = (chan * slots + slot) * 8
                data_rows[at : at + 8, :] = vis[facet, chan, :, slot * LANES : (slot + 1) * LANES].astype(jnp.float32)
        correct(order, where)

    above = layers - 1 - layer
    near_above = above_from - 1 - layer

    last_step = jnp.where(layer <= 1, layers - 3, near_above + 1 + jnp.where(layer < half, layer, 0))
    last_turn = jnp.maximum(above, jnp.minimum(last_step, layers - 1) + LAG)

    def answer(turn, carry):
        @pl.when((turn == 0) & (rank < partner))
        def _():
            pl.semaphore_wait(entered.at[layer], pol_count - 1)
            send(partner, 0)

        @pl.when((turn == 0) & (rank > partner) & (layer >= free))
        def _():
            send(partner, 0)

        @pl.when((turn > 0) & (turn <= above))
        def _():
            with jax.named_scope("hello"):
                pl.semaphore_wait(entered.at[layer + turn], pol_count)

            @pl.when(layer + turn < above_from)
            def _():
                for core in range(pol_count):
                    send((layer + turn) * pol_count + core, 0)

        first = jnp.where(turn == 0, far_below, far_below + turn + 1)
        last = jnp.where(turn < above, jnp.minimum(far_below + turn + 2, layer), jnp.where(turn == above, layer, 0))

        def send_near(low, carry):
            for core in range(pol_count):
                send(low * pol_count + core, 0)
            return carry

        @pl.when(layer < layers - 1)
        def _():
            lax.fori_loop(first, last, send_near, 0)

        @pl.when(turn == above)
        def _():
            send_far()

        @pl.when(layer == layers - 1)
        def _():
            lax.fori_loop(first, last, send_near, 0)

        step = turn - LAG

        @pl.when(turn == last_turn)
        def _():
            answer_last()

        @pl.when(step == 0)
        def _():
            take(rank)
            transfers(partner, pol_count - 1, send_sem, layer).wait_recv()
            take(partner)

        @pl.when(step > 0)
        def _():
            source = jnp.where(step <= near_above, layer + step, step)
            source = jnp.where((step > near_above) & (step <= near_above + layer), step - near_above - 1, source)
            with jax.named_scope("arrive"):
                transfers(source * pol_count, pol_count, send_sem, source).wait_recv()
            with jax.named_scope("correct"):

                def both(core, carry):
                    take(source * pol_count + core)
                    return carry

                lax.fori_loop(0, pol_count, both, 0)

        return carry

    lax.fori_loop(0, layers + LAG, answer, 0)

    with jax.named_scope("finish"):

        @pl.when((layer >= EARLY) & (layer < half))
        def _():
            answers_left()

        @pl.when(layer != 1)
        def _():
            drain()

    with jax.named_scope("order"):
        for f in range(peers):
            out_ref[f] = done[facet_dir_ref[f]]


def shards(gains, visibilities, first_station, second_station, filled_row_count, facet_dir):
    bt_count, pol_count = lax.axis_size("bt"), lax.axis_size("pol")
    peers = bt_count * pol_count
    chans = gains.shape[1]
    hbm = pl.BlockSpec(memory_space=pltpu.HBM)
    vmem = pl.BlockSpec(memory_space=pltpu.VMEM)
    rows = 8 * chans * GAIN_SLOT_COUNT
    operands = (
        facet_dir,
        first_station.reshape(GAIN_SLOT_COUNT, LANES),
        second_station.reshape(GAIN_SLOT_COUNT, LANES),
        gains,
        visibilities,
    )
    return pl.pallas_call(
        functools.partial(kernel, peers, bt_count, pol_count),
        name="correct",
        out_shape=jax.ShapeDtypeStruct(visibilities.shape, visibilities.dtype),
        in_specs=[pl.BlockSpec(memory_space=pltpu.SMEM)] + [hbm] * 5,
        out_specs=vmem,
        scratch_shapes=[
            pltpu.SMEM(facet_dir.shape, jnp.int32),
            pltpu.VMEM((GAIN_SLOT_COUNT, LANES), jnp.int32),
            pltpu.VMEM((GAIN_SLOT_COUNT, LANES), jnp.int32),
            pltpu.VMEM(gains.shape[1:], jnp.float32),
            pltpu.VMEM((peers, TILES, 8, LANES), jnp.float32),
            pltpu.VMEM((peers, TILES, 8, LANES), jnp.float32),
            pltpu.VMEM(visibilities.shape, visibilities.dtype),
            pltpu.VMEM(visibilities.shape, visibilities.dtype),
            pltpu.VMEM((rows, LANES), jnp.float32),
            pltpu.VMEM((rows, LANES), jnp.float32),
            pltpu.VMEM((rows, LANES), jnp.float32),
            pltpu.VMEM((rows, LANES), jnp.float32),
            pltpu.SemaphoreType.DMA((5,)),
            pltpu.SemaphoreType.DMA(((FREE_LAYERS + 1) * pol_count,)),
            pltpu.SemaphoreType.DMA,
            pltpu.SemaphoreType.DMA((bt_count,)),
            pltpu.SemaphoreType.REGULAR((bt_count,)),
            pltpu.SemaphoreType.REGULAR,
        ],
        compiler_params=pltpu.CompilerParams(collective_id=0, has_side_effects=True, vmem_limit_bytes=8 << 20),
    )(filled_row_count, *(pltpu.with_memory_space_constraint(x, pltpu.HBM) for x in operands))


def solution(mesh):
    return jax.shard_map(
        shards,
        mesh=mesh,
        in_specs=(
            P(("obs", "bt", "pol"), "freq", None, None),
            P("obs", "freq", None, ("bt", "pol")),
            P(("obs", "bt", "pol")),
            P(("obs", "bt", "pol")),
            P(("obs", "bt", "pol")),
            P("obs"),
        ),
        out_specs=P("obs", "freq", None, ("bt", "pol")),
        check_vma=False,
    )
```
